128 devices in a mesh: dp: 64 (over z, y, x), cp: 2 (over core).
Axes of the slice: x: 4, y: 4, z: 4, core: 2. Of those that a mesh axis runs over, the one named last changes fastest.
Arguments:
- x: bfloat16 [128, 1024, 1024], P('dp', 'cp')
- grad_out: bfloat16 [128, 1024, 1024], P('dp', 'cp')
- w_q: bfloat16 [1024, 16, 64], replicated
- w_k: bfloat16 [1024, 16, 64], replicated
- w_v: bfloat16 [1024, 16, 64], replicated
- w_o: bfloat16 [1024, 16, 64], replicated
- w_up: bfloat16 [1024, 4096], replicated
- w_down: bfloat16 [4096, 1024], replicated
Outputs:
- output 1: bfloat16 [128, 1024, 1024], P('dp', 'cp')
- output 2: float32 [1024, 16, 64], P(('dp', 'cp'))
- output 3: float32 [1024, 16, 64], P(('dp', 'cp'))
- output 4: float32 [1024, 16, 64], P(('dp', 'cp'))
- output 5: float32 [1024, 16, 64], P(('dp', 'cp'))
- output 6: float32 [1024, 4096], P(('dp', 'cp'))
- output 7: float32 [4096, 1024], P(('dp', 'cp'))
All inputs are finite; a program needn't handle non-finite values.
Results may differ from the reference program's by a relative error of at most 0.0130205.
Values are sent between devices in bfloat16 or wider.
A program may use at most 1 GiB of HBM per device.

```python
import math
import jax
import jax.numpy as jnp
from jax import lax

D_MODEL = 1024
N_HEADS = 16
KV_HEADS = 16
HEAD_DIM = 64
FF_DIM = 4096
CP_SIZE = 2
DP_SIZE = 64
BATCH = 128
SEQ_LEN = 1024
GROUP = N_HEADS // KV_HEADS
HALF = SEQ_LEN // (2 * CP_SIZE)
Q_BLOCK = min(SEQ_LEN, 2 ** max(0, int(math.log2(max(1, 2 ** 22 // (N_HEADS * SEQ_LEN))))))
TOK_BLOCK = min(SEQ_LEN, 2 ** max(0, int(math.log2(max(1, 2 ** 22 // FF_DIM)))))
NEG_BIG = -1e30


def setup_inputs(seed: int = 0) -> dict:
    keys = jax.random.split(jax.random.key(seed), 8)

    def weight(key, shape, fan_in):
        return (jax.random.normal(key, shape, jnp.float32) * fan_in ** -0.5).astype(jnp.bfloat16)

    act_shape = (BATCH, SEQ_LEN, D_MODEL)
    return {
        'x': jax.random.normal(keys[0], act_shape, jnp.float32).astype(jnp.bfloat16),
        'grad_out': jax.random.normal(keys[1], act_shape, jnp.float32).astype(jnp.bfloat16),
        'w_q': weight(keys[2], (D_MODEL, N_HEADS, HEAD_DIM), D_MODEL),
        'w_k': weight(keys[3], (D_MODEL, KV_HEADS, HEAD_DIM), D_MODEL),
        'w_v': weight(keys[4], (D_MODEL, KV_HEADS, HEAD_DIM), D_MODEL),
        'w_o': weight(keys[5], (D_MODEL, N_HEADS, HEAD_DIM), N_HEADS * HEAD_DIM),
        'w_up': weight(keys[6], (D_MODEL, FF_DIM), D_MODEL),
        'w_down': weight(keys[7], (FF_DIM, D_MODEL), FF_DIM),
    }


def to_bf16(values):
    return values.astype(jnp.bfloat16).astype(jnp.float32)


def stored_to_natural(rows):
    blocks = rows.reshape(CP_SIZE, 2, HALF, D_MODEL)
    return jnp.concatenate([blocks[:, 0], blocks[::-1, 1]], axis=0).reshape(SEQ_LEN, D_MODEL)


def natural_to_stored(rows):
    halves = rows.reshape(2, CP_SIZE, HALF, D_MODEL)
    return jnp.stack([halves[0], halves[1][::-1]], axis=1).reshape(SEQ_LEN, D_MODEL)


def layer_row(x_row, w_q, w_k, w_v, w_o, w_up, w_down):
    q_all = to_bf16(jnp.dot(x_row, w_q.reshape(D_MODEL, N_HEADS * HEAD_DIM), preferred_element_type=jnp.float32))
    k_all = to_bf16(jnp.dot(x_row, w_k.reshape(D_MODEL, KV_HEADS * HEAD_DIM), preferred_element_type=jnp.float32)).reshape(SEQ_LEN, KV_HEADS, HEAD_DIM)
    v_all = to_bf16(jnp.dot(x_row, w_v.reshape(D_MODEL, KV_HEADS * HEAD_DIM), preferred_element_type=jnp.float32)).reshape(SEQ_LEN, KV_HEADS, HEAD_DIM)
    q_blocks = q_all.reshape(SEQ_LEN // Q_BLOCK, Q_BLOCK, KV_HEADS, GROUP, HEAD_DIM)
    starts = jnp.arange(SEQ_LEN // Q_BLOCK) * Q_BLOCK
    key_pos = jnp.arange(SEQ_LEN)

    def attn_block(block_in):
        q_blk, start = block_in
        scores = jnp.einsum('qkgd,tkd->kgqt', q_blk, k_all) * HEAD_DIM ** -0.5
        query_pos = start + jnp.arange(Q_BLOCK)
        scores = jnp.where(key_pos[None, :] <= query_pos[:, None], scores, NEG_BIG)
        attn_prob = to_bf16(jax.nn.softmax(scores, axis=-1))
        return to_bf16(jnp.einsum('kgqt,tkd->qkgd', attn_prob, v_all))

    attn_rows = lax.map(jax.checkpoint(attn_block), (q_blocks, starts)).reshape(SEQ_LEN, N_HEADS * HEAD_DIM)
    h_act = to_bf16(x_row + jnp.dot(attn_rows, w_o.reshape(D_MODEL, N_HEADS * HEAD_DIM).T, preferred_element_type=jnp.float32))

    def mlp_block(h_blk):
        hidden = jnp.dot(h_blk, w_up, preferred_element_type=jnp.float32)
        act_out = to_bf16(jax.nn.gelu(hidden, approximate=True))
        return h_blk + jnp.dot(act_out, w_down, preferred_element_type=jnp.float32)

    out_rows = lax.map(jax.checkpoint(mlp_block), h_act.reshape(SEQ_LEN // TOK_BLOCK, TOK_BLOCK, D_MODEL))
    return out_rows.reshape(SEQ_LEN, D_MODEL)


def reference(x, grad_out, w_q, w_k, w_v, w_o, w_up, w_down):
    weights = tuple(weight.astype(jnp.float32) for weight in (w_q, w_k, w_v, w_o, w_up, w_down))

    def row_step(grad_sum, row_pair):
        x_row, cot_row = row_pair
        _, back_fn = jax.vjp(layer_row, stored_to_natural(x_row.astype(jnp.float32)), *weights)
        cotangents = back_fn(stored_to_natural(cot_row.astype(jnp.float32)))
        new_sum = tuple(grad_old + grad_new for grad_old, grad_new in zip(grad_sum, cotangents[1:]))
        return new_sum, natural_to_stored(cotangents[0]).astype(jnp.bfloat16)

    grad_init = tuple(jnp.zeros_like(weight) for weight in weights)
    grad_sums, grad_x = lax.scan(row_step, grad_init, (x, grad_out))
    inv_count = 1.0 / (CP_SIZE * DP_SIZE)
    return (grad_x, grad_sums[0] * inv_count, grad_sums[1] * inv_count, grad_sums[2] * inv_count,
            grad_sums[3] * inv_count, grad_sums[4] * inv_count, grad_sums[5] * inv_count)
```

```python
import jax
import jax.numpy as jnp
from jax import lax
from jax.sharding import PartitionSpec as P

NEG_BIG = -1e30


def gelu_tanh(values):
    return jax.nn.gelu(values, approximate=True)


def solution(mesh):
    cp_size = mesh.shape['cp']
    dev_count = cp_size * mesh.shape['dp']
    swap = [(0, 1), (1, 0)]
    inv = 1.0 / dev_count

    def per_device(x_loc, cot_loc, w_q, w_k, w_v, w_o, w_up, w_down):
        batch, seq_len, d_model = x_loc.shape
        heads, head_dim = w_k.shape[1], w_k.shape[2]
        inner = heads * head_dim
        ff = w_up.shape[1]
        half = seq_len // 2
        tok = 2 * seq_len
        scale = head_dim ** -0.5
        me = lax.axis_index('cp')

        def gather_row(arr):
            mine = lax.dynamic_index_in_dim(arr, me, 0, keepdims=False)
            other = lax.dynamic_index_in_dim(arr, 1 - me, 0, keepdims=False)
            got = lax.ppermute(other, 'cp', swap)
            first = jnp.where(me == 0, mine, got)
            second = jnp.where(me == 0, got, mine)
            return jnp.concatenate([first[:half], second, first[half:]], axis=0)

        x_row = gather_row(x_loc)
        cot = gather_row(cot_loc)
        wq, wk, wv, wo = (w.reshape(d_model, inner) for w in (w_q, w_k, w_v, w_o))

        def dot(a, b, dims):
            return lax.dot_general(a, b, (dims, ((), ())), preferred_element_type=jnp.float32)

        def heads_of(rows):
            return rows.astype(jnp.bfloat16).reshape(tok, heads, head_dim).transpose(1, 0, 2)

        q = heads_of(dot(x_row, wq, ((1,), (0,))))
        k = heads_of(dot(x_row, wk, ((1,), (0,))))
        v = heads_of(dot(x_row, wv, ((1,), (0,))))

        n_blk = 4
        blk = tok // n_blk
        keep = jnp.arange(blk)[None, :] <= jnp.arange(blk)[:, None]

        def scores_of(i):
            s = jnp.einsum('hqe,hte->hqt', q[:, i * blk:(i + 1) * blk], k[:, :(i + 1) * blk], preferred_element_type=jnp.float32) * scale
            mask = jnp.concatenate([jnp.ones((blk, i * blk), bool), keep], axis=1)
            return jnp.where(mask, s, NEG_BIG)

        o_parts, norms = [], []
        for i in range(n_blk):
            s = scores_of(i)
            m = s.max(axis=-1)
            e = jnp.exp(s - m[..., None])
            l = e.sum(axis=-1)
            o = jnp.einsum('hqt,hte->hqe', e.astype(jnp.bfloat16), v[:, :(i + 1) * blk], preferred_element_type=jnp.float32)
            o_parts.append(o / l[..., None])
            norms.append(m + jnp.log(l))
        o_f32 = jnp.concatenate(o_parts, axis=1)
        o_rows = o_f32.astype(jnp.bfloat16).transpose(1, 0, 2).reshape(tok, inner)

        h_act = (x_row + dot(o_rows, wo, ((1,), (1,)))).astype(jnp.bfloat16)
        act_f, gelu_back = jax.vjp(gelu_tanh, dot(h_act, w_up, ((1,), (0,))))
        act_out = act_f.astype(jnp.bfloat16)

        grad_w_down = dot(act_out, cot, ((0,), (0,)))
        grad_act = dot(cot, w_down, ((1,), (1,))).astype(jnp.bfloat16)
        grad_u = gelu_back(grad_act.astype(jnp.float32))[0].astype(jnp.bfloat16)
        grad_w_up = dot(h_act, grad_u, ((0,), (0,)))
        grad_h = cot.astype(jnp.float32) + dot(grad_u, w_up, ((1,), (1,)))
        grad_h_bf = grad_h.astype(jnp.bfloat16)
        grad_w_o = dot(grad_h_bf, o_rows, ((0,), (0,)))

        def shards(g):
            return (g * inv).reshape(dev_count, -1, d_model)

        def reduce(parts):
            joined = jnp.concatenate(parts, axis=1)
            rows = joined.shape[1]
            return lax.psum_scatter(joined.reshape(dev_count * rows, d_model), ('dp', 'cp'), scatter_dimension=0, tiled=True)

        half_ff = ff // 2
        down_shards = shards(grad_w_down)
        up_lo = shards(grad_w_up[:, :half_ff])
        up_hi = shards(grad_w_up[:, half_ff:])
        out_a = reduce([down_shards, up_lo])
        out_b = reduce([up_hi, shards(grad_w_o)])

        grad_o_rows = dot(grad_h_bf, wo, ((1,), (0,)))
        grad_o = heads_of(grad_o_rows)
        delta = jnp.sum(grad_o.astype(jnp.float32) * o_f32, axis=-1)

        dq_parts = []
        dk = [jnp.zeros((heads, blk, head_dim), jnp.float32)] * n_blk
        dv = [jnp.zeros((heads, blk, head_dim), jnp.float32)] * n_blk
        for i in range(n_blk):
            sl = slice(i * blk, (i + 1) * blk)
            p = jnp.exp(scores_of(i) - norms[i][..., None])
            go = grad_o[:, sl]
            kk, vv = k[:, :(i + 1) * blk], v[:, :(i + 1) * blk]
            dvi = jnp.einsum('hqt,hqe->hte', p.astype(jnp.bfloat16), go, preferred_element_type=jnp.float32)
            dp = jnp.einsum('hqe,hte->hqt', go, vv, preferred_element_type=jnp.float32)
            ds = (p * (dp - delta[:, sl][..., None]) * scale).astype(jnp.bfloat16)
            dq_parts.append(jnp.einsum('hqt,hte->hqe', ds, kk, preferred_element_type=jnp.float32))
            dki = jnp.einsum('hqt,hqe->hte', ds, q[:, sl], preferred_element_type=jnp.float32)
            for j in range(i + 1):
                dk[j] = dk[j] + dki[:, j * blk:(j + 1) * blk]
                dv[j] = dv[j] + dvi[:, j * blk:(j + 1) * blk]

        def rows_of(parts):
            return jnp.concatenate(parts, axis=1).astype(jnp.bfloat16).transpose(1, 0, 2).reshape(tok, inner)

        gq, gk, gv = rows_of(dq_parts), rows_of(dk), rows_of(dv)
        out_c = reduce([shards(dot(x_row, g, ((0,), (0,)))) for g in (gq, gk, gv)])

        grad_x = (grad_h + dot(gq, wq, ((1,), (1,))) + dot(gk, wk, ((1,), (1,))) + dot(gv, wv, ((1,), (1,)))).astype(jnp.bfloat16)
        quarter = half
        first = jnp.concatenate([grad_x[:quarter], grad_x[tok - quarter:]], axis=0)
        second = grad_x[quarter:tok - quarter]
        mine = jnp.where(me == 0, first, second)
        other = jnp.where(me == 0, second, first)
        got = lax.ppermute(other, 'cp', swap)
        gx = jnp.stack([jnp.where(me == 0, mine, got), jnp.where(me == 0, got, mine)])

        rows_down = ff // dev_count
        rows = d_model // dev_count
        n_up = rows * half_ff // d_model
        g_down = out_a[:rows_down]
        g_up = jnp.concatenate([out_a[rows_down:].reshape(rows, half_ff), out_b[:n_up].reshape(rows, half_ff)], axis=1)
        g_o = out_b[n_up:].reshape(rows, heads, head_dim)
        g_q, g_k, g_v = (out_c[i * rows:(i + 1) * rows].reshape(rows, heads, head_dim) for i in range(3))
        return gx, g_q, g_k, g_v, g_o, g_up, g_down

    act_spec = P('dp', 'cp', None)
    rep_three = P(None, None, None)
    rep_two = P(None, None)
    grad_three = P(('dp', 'cp'), None, None)
    grad_two = P(('dp', 'cp'), None)
    return jax.shard_map(per_device, mesh=mesh,
                         in_specs=(act_spec, act_spec, rep_three, rep_three, rep_three, rep_three, rep_two, rep_two),
                         out_specs=(act_spec, grad_three, grad_three, grad_three, grad_three, grad_two, grad_two),
                         check_vma=False)
```

```python
import functools
import math

import jax
import jax.numpy as jnp
from jax import lax
from jax.experimental import pallas as pl
from jax.experimental.pallas import tpu as pltpu
from jax.sharding import PartitionSpec as P

F32 = jnp.float32
BF16 = jnp.bfloat16
MESH = pl.DeviceIdType.MESH
NEG_BIG = -1e30
BLK = 256
LANES = 128
RING = 4
CHUNKS = 2
VMEM_MAX = 66_000_000
GELU_C = math.sqrt(2.0 / math.pi)
GELU_A = 0.044715
NN = (((1,), (0,)), ((), ()))
NT = (((1,), (1,)), ((), ()))
TN = (((0,), (0,)), ((), ()))


def dot(a, b, dims=NN):
    return lax.dot_general(a, b, dims, preferred_element_type=F32)


def nat_block(core, i):
    return core if i == 0 else 3 - core


def block_rows(index):
    return pl.ds(pl.multiple_of(index * BLK, BLK), BLK)


def meet(devices):
    barrier = pltpu.get_barrier_semaphore()
    for device in devices:
        pl.semaphore_signal(barrier, inc=1, device_id=device, device_id_type=MESH)
    pl.semaphore_wait(barrier, len(devices))


def qkv_kernel(x_hbm, g_hbm, wq_ref, wk_ref, wv_ref, q_ref, k_ref, v_ref, x_out, g_out, loc_sem, send_sem, recv_sem):
    dp, me = lax.axis_index('dp'), lax.axis_index('cp')
    peer = 1 - me
    pairs = ((x_hbm, x_out), (g_hbm, g_out))
    local = []
    for i, (src, dst) in enumerate(pairs):
        for b in range(2):
            local.append(pltpu.make_async_copy(src.at[me, pl.ds(b * BLK, BLK)], dst.at[block_rows(nat_block(me, b))], loc_sem.at[i, b]))
    for copy in local:
        copy.start()
    meet([(dp, peer)])
    remote = []
    for i, (src, dst) in enumerate(pairs):
        for b in range(2):
            remote.append(pltpu.make_async_remote_copy(
                src.at[peer, pl.ds(b * BLK, BLK)], dst.at[block_rows(nat_block(me, b))],
                send_sem.at[i, b], recv_sem.at[i, b], device_id=(dp, peer), device_id_type=MESH))
    for copy in remote:
        copy.start()

    def project(core):
        rows = [block_rows(nat_block(core, b)) for b in range(2)]
        xs = jnp.concatenate([x_out[r, :] for r in rows], axis=0)
        for w_ref, out in ((wq_ref, q_ref), (wk_ref, k_ref), (wv_ref, v_ref)):
            val = dot(xs, w_ref[...], NT).astype(BF16)
            for b in range(2):
                out[rows[b], :] = val[b * BLK:(b + 1) * BLK]

    local[0].wait()
    local[1].wait()
    project(me)
    remote[0].wait()
    remote[1].wait()
    project(peer)
    for copy in local[2:] + remote[2:]:
        copy.wait()


def qkv_call(x_loc, g_loc, wq, wk, wv):
    rows = 2 * x_loc.shape[1]
    d_model = x_loc.shape[2]
    act = jax.ShapeDtypeStruct((rows, d_model), BF16)
    any_spec = pl.BlockSpec(memory_space=pl.ANY)
    vmem = pl.BlockSpec(memory_space=pltpu.VMEM)
    return pl.pallas_call(
        qkv_kernel,
        out_shape=[act] * 5,
        in_specs=[any_spec] * 2 + [vmem] * 3,
        out_specs=[vmem] * 5,
        scratch_shapes=[pltpu.SemaphoreType.DMA((2, 2))] * 3,
        compiler_params=pltpu.CompilerParams(collective_id=0, has_side_effects=True, vmem_limit_bytes=VMEM_MAX),
        name='qkv',
    )(x_loc, g_loc, wq, wk, wv)


def head_rows(head):
    return lax.broadcasted_iota(jnp.int32, (LANES, 1), 0) // 64 == head


def head_lanes(head):
    return lax.broadcasted_iota(jnp.int32, (1, LANES), 1) // 64 == head


def causal_mask():
    return lax.broadcasted_iota(jnp.int32, (BLK, BLK), 0) <= lax.broadcasted_iota(jnp.int32, (BLK, BLK), 1)


def mask_last(vals, fill):
    last = jnp.where(causal_mask(), vals[-BLK:], fill)
    return last if vals.shape[0] == BLK else jnp.concatenate([vals[:-BLK], last], axis=0)


def attn_fwd_kernel(scale, q_ref, k_ref, v_ref, o_ref, ot_ref, lse_ref):
    to_log2 = scale * math.log2(math.e)
    q_t = q_ref[...].T
    v_t = v_ref[...].T
    for n in range(q_ref.shape[0] // BLK):
        rows = slice(n * BLK, (n + 1) * BLK)
        keys = slice(0, (n + 1) * BLK)
        parts = []
        for head in range(2):
            qz = jnp.where(head_rows(head), q_t[:, rows], jnp.zeros((), BF16))
            st = mask_last(dot(k_ref[keys, :], qz), NEG_BIG)
            top = jnp.max(st, axis=0, keepdims=True) * to_log2
            p = jnp.exp2(st * to_log2 - top)
            total = jnp.sum(p, axis=0, keepdims=True)
            ot = dot(v_t[head * 64:(head + 1) * 64, keys], p.astype(BF16))
            parts.append(ot / total)
            lse_ref[0, head:head + 1, rows] = top + jnp.log2(total)
        both = jnp.concatenate(parts, axis=0)
        ot_ref[:, rows] = both
        o_ref[rows, :] = both.T.astype(BF16)


def attn_fwd_call(q, k, v, scale):
    tok, inner = q.shape
    pairs = inner // LANES
    cols = pl.BlockSpec((tok, LANES), lambda i: (0, i))
    return pl.pallas_call(
        functools.partial(attn_fwd_kernel, scale),
        grid=(pairs,),
        out_shape=[jax.ShapeDtypeStruct((tok, inner), BF16), jax.ShapeDtypeStruct((inner, tok), F32),
                   jax.ShapeDtypeStruct((pairs, 2, tok), F32)],
        in_specs=[cols] * 3,
        out_specs=[cols, pl.BlockSpec((LANES, tok), lambda i: (i, 0)), pl.BlockSpec((1, 2, tok), lambda i: (i, 0, 0))],
        compiler_params=pltpu.CompilerParams(vmem_limit_bytes=VMEM_MAX),
        cost_estimate=pl.CostEstimate(flops=4 * tok * tok * inner, bytes_accessed=12 * tok * inner, transcendentals=0),
        name='attn_fwd',
    )(q, k, v)


def attn_bwd_kernel(scale, q_ref, k_ref, v_ref, go_ref, ot_ref, lse_ref, gq_ref, gk_ref, gv_ref, dk_ref, dv_ref):
    to_log2 = scale * math.log2(math.e)
    zero = jnp.zeros((), BF16)
    q_t = q_ref[...].T
    k_t = k_ref[...].T
    go_t = go_ref[...].T
    n_blk = q_ref.shape[0] // BLK
    for n in reversed(range(n_blk)):
        rows = slice(n * BLK, (n + 1) * BLK)
        keys = slice(0, (n + 1) * BLK)
        p_parts, s_parts, go_parts, q_parts, dq_parts = [], [], [], [], []
        for head in range(2):
            feat = slice(head * 64, (head + 1) * 64)
            qz = jnp.where(head_rows(head), q_t[:, rows], zero)
            goz = jnp.where(head_rows(head), go_t[:, rows], zero)
            st = dot(k_ref[keys, :], qz)
            p = mask_last(jnp.exp2(st * to_log2 - lse_ref[0, head:head + 1, rows]), 0.0)
            dp = dot(v_ref[keys, :], goz)
            delta = jnp.sum(go_t[feat, rows].astype(F32) * ot_ref[feat, rows], axis=0, keepdims=True)
            ds = (p * (dp - delta)).astype(BF16)
            dq_parts.append(dot(k_t[feat, keys], ds))
            p_parts.append(p.astype(BF16))
            s_parts.append(ds)
            go_parts.append(jnp.where(head_lanes(head), go_ref[rows, :], zero))
            q_parts.append(jnp.where(head_lanes(head), q_ref[rows, :], zero))
        gq_ref[rows, :] = (jnp.concatenate(dq_parts, axis=0).T * scale).astype(BF16)
        dv = dot(jnp.concatenate(p_parts, axis=1), jnp.concatenate(go_parts, axis=0))
        dk = dot(jnp.concatenate(s_parts, axis=1), jnp.concatenate(q_parts, axis=0))
        if n == n_blk - 1:
            dv_ref[keys, :] = dv
            dk_ref[keys, :] = dk
        else:
            dv_ref[keys, :] += dv
            dk_ref[keys, :] += dk
    gk_ref[...] = (dk_ref[...] * scale).astype(BF16)
    gv_ref[...] = dv_ref[...].astype(BF16)


def attn_bwd_call(q, k, v, go, ot, lse, scale):
    tok, inner = q.shape
    pairs = inner // LANES
    cols = pl.BlockSpec((tok, LANES), lambda i: (0, i))
    return pl.pallas_call(
        functools.partial(attn_bwd_kernel, scale),
        grid=(pairs,),
        out_shape=[jax.ShapeDtypeStruct((tok, inner), BF16)] * 3,
        in_specs=[cols] * 4 + [pl.BlockSpec((LANES, tok), lambda i: (i, 0)), pl.BlockSpec((1, 2, tok), lambda i: (i, 0, 0))],
        out_specs=[cols] * 3,
        scratch_shapes=[pltpu.VMEM((tok, LANES), F32)] * 2,
        compiler_params=pltpu.CompilerParams(vmem_limit_bytes=VMEM_MAX),
        cost_estimate=pl.CostEstimate(flops=10 * tok * tok * inner, bytes_accessed=18 * tok * inner, transcendentals=0),
        name='attn_bwd',
    )(q, k, v, go, ot, lse)


def split_cores(val, n_dp, me):
    parts = val.reshape(n_dp, 2, val.shape[0] // (2 * n_dp), LANES)
    first, second = parts[:, 0], parts[:, 1]
    mine = me == 0
    return jnp.where(mine, first, second), jnp.where(mine, second, first)


def mlp_kernel(inv, n_dp, x_ref, g_ref, o_ref, wo_ref, up_ref, down_ref, dn_keep, dn_send, up_keep, up_send, o_keep, o_send,
               gh_out, go_out, h_ref, gh_ref):
    me = lax.axis_index('cp')
    step = pl.program_id(0)
    d_model = x_ref.shape[1]
    width = up_ref.shape[1]

    @pl.when(step == 0)
    def _():
        h_ref[...] = (x_ref[...].astype(F32) + dot(o_ref[...], wo_ref[...])).astype(BF16)
        gh_ref[...] = g_ref[...].astype(F32)

    u = dot(h_ref[...], up_ref[...])
    ga = dot(g_ref[...], down_ref[...], NT).astype(BF16).astype(F32)
    u2 = u * u
    t = jnp.tanh(u * (GELU_C + (GELU_C * GELU_A) * u2))
    half_t = 0.5 * (1.0 + t)
    act = (u * half_t).astype(BF16)
    slope = half_t + (0.5 * u) * ((1.0 - t) * (1.0 + t)) * (GELU_C + (3.0 * GELU_C * GELU_A) * u2)
    gu = (ga * slope).astype(BF16)

    dn = dot(act, g_ref[...], TN) * inv
    n_here = dn_keep.shape[0]
    for j in range(d_model // LANES):
        keep, send = split_cores(dn[:, j * LANES:(j + 1) * LANES], n_here, me)
        dn_keep[:, :, j] = keep.reshape(n_here, -1, 8, LANES)
        dn_send[:, :, j] = send.reshape(n_here, -1, 8, LANES)

    up = dot(h_ref[...], gu, TN) * inv
    for j in range(width // LANES):
        keep, send = split_cores(up[:, j * LANES:(j + 1) * LANES], n_dp, me)
        up_keep[:, j] = keep
        up_send[:, j] = send

    gh_ref[...] += dot(gu, up_ref[...], NT)

    @pl.when(step == pl.num_programs(0) - 1)
    def _():
        gh_out[...] = gh_ref[...]
        ghb = gh_ref[...].astype(BF16)
        dwo = dot(ghb, o_ref[...], TN) * inv
        for j in range(dwo.shape[1] // LANES):
            keep, send = split_cores(dwo[:, j * LANES:(j + 1) * LANES], n_dp, me)
            o_keep[:, j] = keep
            o_send[:, j] = send
        go_out[...] = dot(ghb, wo_ref[...], NT).astype(BF16)


def mlp_call(x, g, o, wo, w_up, w_down, n_dp, inv):
    tok, d_model = x.shape
    ff = w_up.shape[1]
    width = 512
    steps = ff // width
    whole = pl.BlockSpec((tok, d_model), lambda i: (0, 0), pipeline_mode=pl.Buffered(1))
    down = jax.ShapeDtypeStruct((n_dp, ff // (2 * n_dp * 8), d_model // LANES, 8, LANES), F32)
    up = jax.ShapeDtypeStruct((n_dp, ff // LANES, 8, LANES), F32)
    out = jax.ShapeDtypeStruct((n_dp, d_model // LANES, 8, LANES), F32)
    down_spec = pl.BlockSpec((n_dp // steps,) + down.shape[1:], lambda i: (i, 0, 0, 0, 0))
    up_spec = pl.BlockSpec((n_dp, width // LANES, 8, LANES), lambda i: (0, i, 0, 0))
    out_spec = pl.BlockSpec(out.shape, lambda i: (0, 0, 0, 0), pipeline_mode=pl.Buffered(1))
    return pl.pallas_call(
        functools.partial(mlp_kernel, inv, n_dp),
        grid=(steps,),
        out_shape=[down, down, up, up, out, out, jax.ShapeDtypeStruct((tok, d_model), F32),
                   jax.ShapeDtypeStruct((tok, d_model), BF16)],
        in_specs=[whole] * 4 + [pl.BlockSpec((d_model, width), lambda i: (0, i)), pl.BlockSpec((width, d_model), lambda i: (i, 0))],
        out_specs=[down_spec, down_spec, up_spec, up_spec, out_spec, out_spec, whole, whole],
        scratch_shapes=[pltpu.VMEM((tok, d_model), BF16), pltpu.VMEM((tok, d_model), F32)],
        compiler_params=pltpu.CompilerParams(vmem_limit_bytes=VMEM_MAX),
        cost_estimate=pl.CostEstimate(flops=10 * tok * d_model * ff, bytes_accessed=4 * 2 * d_model * ff, transcendentals=0),
        name='mlp',
    )(x, g, o, wo, w_up, w_down)


def dqkv_kernel(inv, n_dp, x_ref, gq_ref, gk_ref, gv_ref, keep_ref, send_ref):
    me = lax.axis_index('cp')
    for i, ref in enumerate((gq_ref, gk_ref, gv_ref)):
        dw = dot(x_ref[...], ref[...], TN) * inv
        for j in range(dw.shape[1] // LANES):
            keep, send = split_cores(dw[:, j * LANES:(j + 1) * LANES], n_dp, me)
            keep_ref[:, i, j] = keep
            send_ref[:, i, j] = send


def dqkv_call(x, gq, gk, gv, n_dp, inv):
    tok, d_model = x.shape
    inner = gq.shape[1]
    width = 256
    whole = pl.BlockSpec((tok, d_model), lambda i: (0, 0), pipeline_mode=pl.Buffered(1))
    cols = pl.BlockSpec((tok, width), lambda i: (0, i))
    out = jax.ShapeDtypeStruct((n_dp, 3, inner // LANES, 8, LANES), F32)
    spec = pl.BlockSpec((n_dp, 3, width // LANES, 8, LANES), lambda i: (0, 0, i, 0, 0))
    return pl.pallas_call(
        functools.partial(dqkv_kernel, inv, n_dp),
        grid=(inner // width,),
        out_shape=[out, out],
        in_specs=[whole, cols, cols, cols],
        out_specs=[spec, spec],
        compiler_params=pltpu.CompilerParams(vmem_limit_bytes=VMEM_MAX),
        cost_estimate=pl.CostEstimate(flops=6 * tok * d_model * inner, bytes_accessed=12 * d_model * inner, transcendentals=0),
        name='dqkv',
    )(x, gq, gk, gv)


def gx_kernel(gq_ref, gk_ref, gv_ref, wq_ref, wk_ref, wv_ref, gh_ref, out_hbm, stage, loc_sem, send_sem, recv_sem):
    dp, me = lax.axis_index('dp'), lax.axis_index('cp')
    peer = 1 - me
    meet([(dp, peer)])

    def rows_of(core, slot):
        rows = [block_rows(nat_block(core, b)) for b in range(2)]

        def both(ref):
            return jnp.concatenate([ref[r, :] for r in rows], axis=0)

        total = both(gh_ref)
        for ref, w_ref in ((gq_ref, wq_ref), (gk_ref, wk_ref), (gv_ref, wv_ref)):
            total += dot(both(ref), w_ref[...])
        stage[slot] = total.astype(BF16)

    rows_of(peer, 0)
    away = pltpu.make_async_remote_copy(stage.at[0], out_hbm.at[me], send_sem, recv_sem, device_id=(dp, peer), device_id_type=MESH)
    away.start()
    rows_of(me, 1)
    home = pltpu.make_async_copy(stage.at[1], out_hbm.at[me], loc_sem)
    home.start()
    home.wait()
    away.wait()


def gx_call(gq, gk, gv, wq, wk, wv, gh):
    tok, d_model = gh.shape
    vmem = pl.BlockSpec(memory_space=pltpu.VMEM)
    return pl.pallas_call(
        gx_kernel,
        out_shape=jax.ShapeDtypeStruct((2, tok // 2, d_model), BF16),
        in_specs=[vmem] * 7,
        out_specs=pl.BlockSpec(memory_space=pl.ANY),
        scratch_shapes=[pltpu.VMEM((2, tok // 2, d_model), BF16)] + [pltpu.SemaphoreType.DMA] * 3,
        compiler_params=pltpu.CompilerParams(collective_id=1, has_side_effects=True, vmem_limit_bytes=VMEM_MAX),
        name='gx',
    )(gq, gk, gv, wq, wk, wv, gh)


class Color:
    def __init__(self, axes, chunks):
        self.axes = axes
        self.chunks = chunks


def rs_plan():
    down = [[(0, i * 128, 128)] for i in range(2)]
    up = [[(1, i * 128, 128)] for i in range(2)]
    attn = [[(2, 0, 64), (3, 0, 64)], [(3, 64, 128)]]
    return [Color((2, 1, 0), down), Color((1, 0, 2), up), Color((0, 2, 1), attn)]


def rs_kernel(plan, *refs):
    n_in = 1 + max(piece[0] for color in plan for chunk in color.chunks for piece in chunk)
    keep, recv, out_ref = refs[:n_in], refs[n_in:2 * n_in], refs[2 * n_in]
    own, tmp, r1a, r1b, r2a, r2b, r3a, r3b, keep_sem, part_sem, send_sem, recv_sem = refs[2 * n_in + 1:]
    got = ((r1a, r1b), (r2a, r2b), (r3a, r3b))
    rows = own.shape[5]
    half = rows // 2
    dp, cp = lax.axis_index('dp'), lax.axis_index('cp')
    coords = (dp // 16, (dp // 4) % 4, dp % 4)

    def neighbor(axis, delta):
        at = list(coords)
        at[axis] = (coords[axis] + delta) % RING
        return (at[0] * 16 + at[1] * 4 + at[2], cp)

    def group(color, phase, delta):
        index = [slice(None)] * 3
        for axis in color.axes[:phase]:
            index[axis] = coords[axis]
        axis = color.axes[phase]
        index[axis] = (coords[axis] + delta) % RING
        return tuple(index)

    def add_into(dst, index, srcs, first, count):
        open_dims = [i for i, entry in enumerate(index) if isinstance(entry, slice)]
        where = pl.ds(first, count)

        def at(i):
            full = list(index)
            inner = []
            for position, dim in enumerate(open_dims):
                rank = len(open_dims) - 1 - position
                entry = (i // RING ** rank) % RING
                full[dim] = entry
                inner.append(entry)
            return tuple(full), tuple(inner)

        def body(i, carry):
            full, inner = at(i)
            total = dst[full + (where, slice(None))]
            for src in srcs:
                total += src[inner]
            dst[full + (where, slice(None))] = total
            return carry

        trips = RING ** len(open_dims)
        if trips == 1:
            body(0, 0)
        else:
            lax.fori_loop(0, trips, body, 0)

    order = (2, 1, 3, 0)
    units = [(q, c) for q in range(len(plan[0].chunks)) for c in range(len(plan))]
    keep_copies, part_copies = {}, {}
    slot = 0
    for delta in order:
        for q, c in units:
            index = group(plan[c], 0, delta)
            at = 0
            pieces = []
            for number, (which, first, count) in enumerate(plan[c].chunks[q]):
                span = (pl.ds(first, count), slice(None))
                pieces.append((pltpu.make_async_copy(keep[which].at[index + span], own.at[(c, q) + index + (pl.ds(at, count), slice(None))],
                                                     keep_sem.at[c, q, delta, number]),
                               pltpu.make_async_copy(recv[which].at[index + span], tmp.at[(slot % tmp.shape[0], slice(None), slice(None), pl.ds(at, count), slice(None))],
                                                     part_sem.at[c, q, delta, number])))
                at += count
            keep_copies[q, c, delta] = [p[0] for p in pieces]
            part_copies[q, c, delta] = ([p[1] for p in pieces], slot % tmp.shape[0])
            slot += 1
    for delta in order:
        for q, c in units:
            for copy in keep_copies[q, c, delta]:
                copy.start()
    queue = [(q, c, delta) for delta in order for q, c in units]
    for key in queue[:tmp.shape[0]]:
        for copy in part_copies[key][0]:
            copy.start()
    ahead = list(queue[tmp.shape[0]:])

    def take(q, c, delta):
        copies, where = part_copies[q, c, delta]
        for copy in keep_copies[q, c, delta] + copies:
            copy.wait()
        add_into(own.at[c, q], group(plan[c], 0, delta), [tmp.at[where]], 0, rows)
        if ahead:
            for copy in part_copies[ahead.pop(0)][0]:
                copy.start()

    sends = []

    def send(q, c, phase, step):
        axis = plan[c].axes[phase]
        pair = []
        for way, sign in enumerate((1, -1)):
            target = group(plan[c], phase, 2 if step == 0 else sign)
            span = pl.ds(way * half, half) if step == 0 else slice(None)
            copy = pltpu.make_async_remote_copy(
                own.at[(c, q) + target + (span, slice(None))], got[phase][step].at[c, q, way],
                send_sem.at[c, q, phase, step, way], recv_sem.at[c, q, phase, step, way],
                device_id=neighbor(axis, sign), device_id_type=MESH)
            copy.start()
            pair.append(copy)
        sends.extend(pair)
        return pair

    def land(copies, q, c, phase, step):
        for copy in copies:
            copy.wait_recv()
        bufs = [got[phase][step].at[c, q, way] for way in range(2)]
        if step == 0:
            for way, sign in enumerate((1, -1)):
                add_into(own.at[c, q], group(plan[c], phase, sign), [bufs[way]], way * half, half)
        else:
            add_into(own.at[c, q], group(plan[c], phase, 0), bufs, 0, rows)

    meet([neighbor(axis, sign) for axis in range(3) for sign in (1, -1)])
    flying = {}
    for q, c in units:
        take(q, c, 2)
        flying[q, c] = send(q, c, 0, 0)
    for delta in (1, 3, 0):
        for q, c in units:
            take(q, c, delta)
    for phase in range(3):
        for q, c in units:
            land(flying[q, c], q, c, phase, 0)
            flying[q, c] = send(q, c, phase, 1)
        for q, c in units:
            land(flying[q, c], q, c, phase, 1)
            if phase < 2:
                flying[q, c] = send(q, c, phase + 1, 0)
            else:
                out_ref[c, pl.ds(q * rows, rows), :] = own[(c, q) + coords]
    for copy in sends:
        copy.wait_send()


def rs_call(keep, recv):
    plan = rs_plan()
    colors, chunks = len(plan), len(plan[0].chunks)
    rows = sum(piece[2] for piece in plan[0].chunks[0])
    half = rows // 2
    any_spec = pl.BlockSpec(memory_space=pl.ANY)
    lead = (colors, chunks, 2)
    got = []
    for dims in ((RING, RING), (RING,), ()):
        got += [pltpu.VMEM(lead + dims + (half, LANES), F32), pltpu.VMEM(lead + dims + (rows, LANES), F32)]
    return pl.pallas_call(
        functools.partial(rs_kernel, plan),
        out_shape=jax.ShapeDtypeStruct((colors, chunks * rows, LANES), F32),
        in_specs=[any_spec] * (len(keep) + len(recv)),
        out_specs=pl.BlockSpec(memory_space=pltpu.VMEM),
        scratch_shapes=[pltpu.VMEM((colors, chunks, RING, RING, RING, rows, LANES), F32), pltpu.VMEM((4, RING, RING, rows, LANES), F32)] + got + [
            pltpu.SemaphoreType.DMA((colors, chunks, RING, 2)), pltpu.SemaphoreType.DMA((colors, chunks, RING, 2)),
            pltpu.SemaphoreType.DMA((colors, chunks, 3, 2, 2)), pltpu.SemaphoreType.DMA((colors, chunks, 3, 2, 2))],
        compiler_params=pltpu.CompilerParams(collective_id=2, has_side_effects=True, vmem_limit_bytes=VMEM_MAX),
        name='rs',
    )(*keep, *recv)


def solution(mesh):
    n_dp = mesh.shape['dp']
    dev_count = mesh.shape['cp'] * n_dp
    inv = 1.0 / dev_count
    swap = [(0, 1), (1, 0)]

    def per_device(x_loc, cot_loc, w_q, w_k, w_v, w_o, w_up, w_down):
        d_model, heads, head_dim = w_q.shape
        inner = heads * head_dim
        ff = w_up.shape[1]
        scale = head_dim ** -0.5
        wq, wk, wv, wo = (w.transpose(1, 2, 0).reshape(inner, d_model) for w in (w_q, w_k, w_v, w_o))

        q, k, v, x, g = qkv_call(x_loc, cot_loc, wq, wk, wv)
        o, ot, lse = attn_fwd_call(q, k, v, scale)
        dn_keep, dn_send, up_keep, up_send, o_keep, o_send, gh, go = mlp_call(x, g, o, wo, w_up, w_down, n_dp, inv)
        gq, gk, gv = attn_bwd_call(q, k, v, go, ot, lse, scale)
        qkv_keep, qkv_send = dqkv_call(x, gq, gk, gv, n_dp, inv)
        gx = gx_call(gq, gk, gv, wq, wk, wv, gh)

        def view(arr):
            return arr.reshape(RING, RING, RING, -1, LANES)

        keep = [view(a) for a in (dn_keep, up_keep, o_keep, qkv_keep)]
        recv = [lax.ppermute(view(a), 'cp', swap) for a in (dn_send, up_send, o_send, qkv_send)]
        out = rs_call(keep, recv)

        rows = d_model // dev_count
        g_down = out[0].reshape(-1, d_model // LANES, 8, LANES).transpose(0, 2, 1, 3).reshape(ff // dev_count, d_model)
        g_up = out[1].reshape(ff // LANES, rows, LANES).transpose(1, 0, 2).reshape(rows, ff)
        g_attn = out[2].reshape(4, inner // LANES, rows, LANES).transpose(0, 2, 1, 3).reshape(4, rows, heads, head_dim)
        return gx, g_attn[1], g_attn[2], g_attn[3], g_attn[0], g_up, g_down

    act_spec = P('dp', 'cp', None)
    rep_three = P(None, None, None)
    rep_two = P(None, None)
    grad_three = P(('dp', 'cp'), None, None)
    grad_two = P(('dp', 'cp'), None)
    return jax.shard_map(per_device, mesh=mesh,
                         in_specs=(act_spec, act_spec, rep_three, rep_three, rep_three, rep_three, rep_two, rep_two),
                         out_specs=(act_spec, grad_three, grad_three, grad_three, grad_three, grad_two, grad_two),
                         check_vma=False)
```
